32 devices in a mesh: replica: 8 (over z, y), model: 4 (over x, core).
Axes of the slice: x: 2, y: 2, z: 4, core: 2. Of those that a mesh axis runs over, the one named last changes fastest.
Arguments:
- partial_up: float32 [8, 1024, 4096], P('replica', None, 'model'), may hold values from -4 to 4
- partial_down: float32 [8, 4096, 1024], P('replica', 'model'), may hold values from -4 to 4
- partial_norm: float32 [8, 1024], P('replica'), may hold values from -8 to 8
- partial_bias: float32 [8, 1024], P('replica'), may hold values from -8 to 8
- master_up: float32 [1024, 4096], P('replica', 'model'), may hold values from -0.1875 to 0.1875
- master_down: float32 [4096, 1024], P('model', 'replica'), may hold values from -0.09375 to 0.09375
- master_norm: float32 [1024], P('replica'), may hold values from 0.25 to 1.75
- master_bias: float32 [1024], P('replica'), may hold values from -3 to 3
- memory_up: float32 [1024, 4096], P('replica', 'model'), may hold values from 0.05 to 0.8
- memory_down: float32 [4096, 1024], P('model', 'replica'), may hold values from 0.05 to 0.8
- memory_norm: float32 [1024], P('replica'), may hold values from 0.05 to 0.8
- memory_bias: float32 [1024], P('replica'), may hold values from 0.05 to 0.8
Outputs:
- compute_up: bfloat16 [1024, 4096], P(None, 'model')
- compute_down: bfloat16 [4096, 1024], P('model')
- compute_norm: bfloat16 [1024], replicated
- compute_bias: bfloat16 [1024], replicated
- stepped_up: float32 [1024, 4096], P('replica', 'model')
- stepped_down: float32 [4096, 1024], P('model', 'replica')
- stepped_norm: float32 [1024], P('replica')
- stepped_bias: float32 [1024], P('replica')
- state_new_up: float32 [1024, 4096], P('replica', 'model')
- state_new_down: float32 [4096, 1024], P('model', 'replica')
- state_new_norm: float32 [1024], P('replica')
- state_new_bias: float32 [1024], P('replica')
The draws below stay inside these ranges and needn't reach their ends.
All inputs are finite; a program needn't handle non-finite values.
Results may differ from the reference program's by a relative error of at most 0.001.
Values may be sent and summed in bfloat16 or wider, within the bound.
A program may use at most 128 MiB of HBM per device.

```python
import jax
import jax.numpy as jnp
from jax import lax

WIDTH = 1024
INNER = 4096
REPLICAS = 8


def spiked(result, key, source, target, parts, factor):
    owner, partner = [(jnp.arange(result.shape[dim]) // (result.shape[dim] // parts)).reshape([-1 if axis == dim else 1 for axis in range(result.ndim)]) for dim in (source, target)]
    chosen = jax.random.permutation(key, parts)[partner]
    strong = (owner == chosen) | (owner == (partner + parts // 2) % parts)
    return jnp.where(strong, factor * result, result)


def steps_of(own_key, extent, split, low, high):
    gain = 1.0
    for dim, shards_of in split:
        heights = jax.random.uniform(jax.random.fold_in(jax.random.fold_in(own_key, 6), dim), (shards_of,), jnp.float32, low / len(split), high / len(split))
        gain = gain * jnp.repeat(jnp.exp(heights), extent[dim] // shards_of).reshape((-1,) + (1,) * (len(extent) - 1 - dim))
    return gain


def bell_draw(own_key, extent, width, limit, shards=(), kind=jnp.bfloat16):
    factor_of = steps_of(own_key, extent, shards, -0.22, 0.18) if shards else 1.0
    array = jax.random.normal(own_key, extent, jnp.float32) * width * factor_of
    return jnp.minimum(jnp.maximum(array, -limit), limit).astype(kind)


def heavy_noise(rng, extent, width, reach, cuts, heavy, held_as=jnp.bfloat16):
    entries = width * jax.random.normal(rng, extent, jnp.float32)
    if cuts:
        entries = entries * steps_of(rng, extent, cuts, -0.22, 0.18)
    return jnp.clip(spiked(entries, jax.random.fold_in(rng, 3), *heavy), -reach, reach).astype(held_as)


def setup_inputs(seed: int = 0) -> dict:
    arg_keys = jax.random.split(jax.random.key(seed), 13)
    return {
        "partial_up": heavy_noise(arg_keys[0], (REPLICAS, WIDTH, INNER), 0.5, 4.0, ((0, 8), (2, 4)), (0, 1, 8, 2.0), jnp.float32),
        "partial_down": heavy_noise(arg_keys[1], (REPLICAS, INNER, WIDTH), 0.5, 4.0, ((0, 8), (1, 4)), (0, 2, 8, 2.0), jnp.float32),
        "partial_norm": heavy_noise(arg_keys[2], (REPLICAS, WIDTH), 1.0, 8.0, ((0, 8),), (0, 1, 8, 2.0), jnp.float32),
        "partial_bias": heavy_noise(arg_keys[3], (REPLICAS, WIDTH), 1.0, 8.0, ((0, 8),), (0, 1, 8, 2.0), jnp.float32),
        "master_up": bell_draw(arg_keys[4], (WIDTH, INNER), WIDTH ** -0.5, 0.1875, ((0, 8), (1, 4)), jnp.float32),
        "master_down": bell_draw(arg_keys[5], (INNER, WIDTH), INNER ** -0.5, 0.09375, ((0, 4), (1, 8)), jnp.float32),
        "master_norm": jnp.clip(1.0 + 0.15 * jax.random.normal(arg_keys[6], (WIDTH,), jnp.float32), 0.25, 1.75),
        "master_bias": bell_draw(arg_keys[7], (WIDTH,), 0.5, 3.0, ((0, 8),), jnp.float32),
        "memory_up": jnp.clip(0.05 + 0.75 * jax.random.uniform(arg_keys[8], (WIDTH, INNER), jnp.float32) ** steps_of(arg_keys[8], (WIDTH, INNER), ((0, 8), (1, 4)), -0.2, 0.2), 0.05, 0.8),
        "memory_down": jnp.clip(0.05 + 0.75 * jax.random.uniform(arg_keys[9], (INNER, WIDTH), jnp.float32) ** steps_of(arg_keys[9], (INNER, WIDTH), ((0, 4), (1, 8)), -0.2, 0.2), 0.05, 0.8),
        "memory_norm": jnp.clip(0.05 + 0.75 * jax.random.uniform(arg_keys[10], (WIDTH,), jnp.float32) ** steps_of(arg_keys[10], (WIDTH,), ((0, 8),), -0.2, 0.2), 0.05, 0.8),
        "memory_bias": jnp.clip(0.05 + 0.75 * jax.random.uniform(arg_keys[11], (WIDTH,), jnp.float32) ** steps_of(arg_keys[11], (WIDTH,), ((0, 8),), -0.2, 0.2), 0.05, 0.8),
    }


learn_rate = 0.05
hold_rate = 0.9

def reference(partial_up, partial_down, partial_norm, partial_bias, master_up, master_down, master_norm, master_bias, memory_up, memory_down, memory_norm, memory_bias):
    mean_up = lax.optimization_barrier(jnp.sum(partial_up.astype(jnp.float32), axis=0)) * REPLICAS ** (-0.5)
    mean_down = lax.optimization_barrier(jnp.sum(partial_down.astype(jnp.float32), axis=0)) * REPLICAS ** (-0.5)
    mean_norm = lax.optimization_barrier(jnp.sum(partial_norm.astype(jnp.float32), axis=0)) * REPLICAS ** (-0.5)
    mean_bias = lax.optimization_barrier(jnp.sum(partial_bias.astype(jnp.float32), axis=0)) * REPLICAS ** (-0.5)
    state_new_up = hold_rate * memory_up + (1.0 - hold_rate) * mean_up * mean_up
    stepped_up = master_up - learn_rate * mean_up * lax.rsqrt(state_new_up + 1e-06)
    state_new_down = hold_rate * memory_down + (1.0 - hold_rate) * mean_down * mean_down
    stepped_down = master_down - learn_rate * mean_down * lax.rsqrt(state_new_down + 1e-06)
    state_new_norm = hold_rate * memory_norm + (1.0 - hold_rate) * mean_norm * mean_norm
    stepped_norm = master_norm - learn_rate * mean_norm * lax.rsqrt(state_new_norm + 1e-06)
    state_new_bias = hold_rate * memory_bias + (1.0 - hold_rate) * mean_bias * mean_bias
    stepped_bias = master_bias - learn_rate * mean_bias * lax.rsqrt(state_new_bias + 1e-06)
    compute_up = stepped_up.astype(jnp.bfloat16)
    compute_down = stepped_down.astype(jnp.bfloat16)
    compute_norm = stepped_norm.astype(jnp.bfloat16)
    compute_bias = stepped_bias.astype(jnp.bfloat16)
    return (compute_up, compute_down, compute_norm, compute_bias, stepped_up, stepped_down, stepped_norm, stepped_bias, state_new_up, state_new_down, state_new_norm, state_new_bias)
```

```python
import functools
import math

import jax
import jax.numpy as jnp
from jax import lax
from jax.experimental import pallas as pl
from jax.experimental.pallas import tpu as pltpu
from jax.sharding import PartitionSpec as P

learn_rate = 0.05
hold_rate = 0.9


def plain(
    partial_up,
    partial_down,
    partial_norm,
    partial_bias,
    master_up,
    master_down,
    master_norm,
    master_bias,
    memory_up,
    memory_down,
    memory_norm,
    memory_bias,
):
    mean_up, mean_down = (
        lax.psum_scatter(partial_up[0], "replica", scatter_dimension=0, tiled=True),
        lax.psum_scatter(partial_down[0], "replica", scatter_dimension=1, tiled=True),
    )
    whole_norm, whole_bias = lax.psum((partial_norm[0], partial_bias[0]), "replica")
    place = lax.axis_index("replica")
    mean_norm = lax.dynamic_slice_in_dim(
        whole_norm, place * master_norm.shape[0], master_norm.shape[0]
    )
    mean_bias = lax.dynamic_slice_in_dim(
        whole_bias, place * master_bias.shape[0], master_bias.shape[0]
    )
    mean_rate = lax.axis_size("replica") ** (-0.5)
    mean_up = mean_up * mean_rate
    mean_down = mean_down * mean_rate
    mean_norm = mean_norm * mean_rate
    mean_bias = mean_bias * mean_rate
    state_new_up = hold_rate * memory_up + (1.0 - hold_rate) * mean_up * mean_up
    stepped_up = master_up - learn_rate * mean_up * lax.rsqrt(state_new_up + 1e-06)
    state_new_down = hold_rate * memory_down + (1.0 - hold_rate) * mean_down * mean_down
    stepped_down = master_down - learn_rate * mean_down * lax.rsqrt(state_new_down + 1e-06)
    state_new_norm = hold_rate * memory_norm + (1.0 - hold_rate) * mean_norm * mean_norm
    stepped_norm = master_norm - learn_rate * mean_norm * lax.rsqrt(state_new_norm + 1e-06)
    state_new_bias = hold_rate * memory_bias + (1.0 - hold_rate) * mean_bias * mean_bias
    stepped_bias = master_bias - learn_rate * mean_bias * lax.rsqrt(state_new_bias + 1e-06)
    compute_up, compute_down, compute_norm, compute_bias = (
        lax.all_gather(stepped_up.astype(jnp.bfloat16), "replica", axis=0, tiled=True),
        lax.all_gather(stepped_down.astype(jnp.bfloat16), "replica", axis=1, tiled=True),
        lax.all_gather(stepped_norm.astype(jnp.bfloat16), "replica", axis=0, tiled=True),
        lax.all_gather(stepped_bias.astype(jnp.bfloat16), "replica", axis=0, tiled=True),
    )
    return (
        compute_up,
        compute_down,
        compute_norm,
        compute_bias,
        stepped_up,
        stepped_down,
        stepped_norm,
        stepped_bias,
        state_new_up,
        state_new_down,
        state_new_norm,
        state_new_bias,
    )


HALVES = 2
SHARE = 5 / 8
SPAN = 124.0
POWER = 49
STEEP = 2.0 ** (2.0 * SPAN / POWER) - 1.0
LOW = 2.0 ** (-SPAN / POWER)
LAG_PAIR = 4
LAG_SUM = 2
LAG_GATHER = 2
LAG_SIDE = 2
LAG_VECTOR = 4


def encode(x, reach):
    q = x * (LOW * STEEP / reach) + jnp.where(x < 0.0, -LOW, LOW)
    q2 = q * q
    q3 = q2 * q
    q6 = q3 * q3
    q12 = q6 * q6
    q24 = q12 * q12
    q48 = q24 * q24
    return (q48 * q).astype(jnp.bfloat16)


def decode(code, reach):
    y = code.astype(jnp.float32)
    grown = jnp.exp2(jnp.log(jnp.abs(y)) * (1.0 / (math.log(2.0) * POWER)))
    scale = reach / (LOW * STEEP)
    return (grown - LOW) * jnp.where(y < 0.0, -scale, scale)


def update(total, master, memory, rate):
    mean = total * rate
    state = hold_rate * memory + (1.0 - hold_rate) * mean * mean
    return master - learn_rate * mean * lax.rsqrt(state + 1e-06), state


def shares(hb):
    size = hb // HALVES
    first = int(size * SHARE) // 8 * 8
    return size, first, size - first


def kernel(
    n,
    pu, pd, mu, md, su, sd, pn, pb, mn, mb, sn, sb,
    gy, gz, ou, od, qu, qd, cn, cb, step_s, state_s,
    xs, wu, wd, hu, hd,
    a_s, a_r, c_s0, c_s1, c_r0, c_r1, z_s0, z_s1, z_r0, z_r1, y_s, y_r,
    mine, theirs, packs, hold_s,
    sem_up, sem_down, sem_par, sem_vec,
    sa, ra, sc, rc, sz, rz, sy, ry, so, ro, st, rt, sf, rf, sg, rg, sp, rp, sq, rq, sv, rv, sw, rw,
):
    H = HALVES
    nz = n // 2
    tiles, _, hb, wide = xs.shape
    size, part_y, part_z = shares(hb)
    tiles_up = pu.shape[2] // wide
    units = tiles * H
    me = lax.axis_index("replica")
    y = lax.rem(me, 2)
    row = lax.div(me, 2)
    other = me + 1 - 2 * y
    rate = n ** (-0.5)
    reach = n / 2.0
    c_s, c_r, z_s, z_r = (c_s0, c_s1), (c_r0, c_r1), (z_s0, z_s1), (z_r0, z_r1)

    def remote(src, dst, ss, rs, who):
        return pltpu.make_async_remote_copy(
            src_ref=src, dst_ref=dst, send_sem=ss, recv_sem=rs,
            device_id={"replica": who}, device_id_type=pl.DeviceIdType.MESH,
        )

    def load_up(k):
        lanes = pl.ds(pl.multiple_of(k * wide, wide), wide)
        return pltpu.make_async_copy(pu.at[:, :, lanes], xs.at[k], sem_up.at[k])

    def load_down(b):
        return pltpu.make_async_copy(
            pd.at[:, :, b * wide : (b + 1) * wide], xs.at[tiles_up:tiles, b], sem_down.at[b]
        )

    params = [
        pltpu.make_async_copy(a, b, sem_par.at[i])
        for i, (a, b) in enumerate(((mu, wu), (su, hu), (md, wd), (sd, hd)))
    ]
    vectors = [
        pltpu.make_async_copy(a, mine.at[at : at + a.shape[0], :], sem_vec.at[i])
        for i, (a, at) in enumerate(
            ((pn, 0), (pb, n), (mn, 2 * n), (mb, 2 * n + 1), (sn, 2 * n + 2), (sb, 2 * n + 3))
        )
    ]

    def tile_of(u):
        return lax.div(u, H), lax.rem(u, H)

    def rows_y(half):
        return pl.ds(pl.multiple_of(half * size, 8), part_y)

    def rows_z(half):
        return pl.ds(pl.multiple_of(half * size + part_y, 8), part_z)

    def encode_a(u):
        k, half = tile_of(u)

        @pl.when(jnp.logical_and(half == 0, k < tiles_up))
        def _():
            load_up(k).wait()

        @pl.when(u == tiles_up * H)
        def _():
            for b in range(n):
                load_down(b).wait()

        for t in range(nz):
            a_s[u, t] = encode(xs[k, 2 * t + 1 - y, rows_y(half), :], reach)

    load_up(0).start()
    barrier = pltpu.get_barrier_semaphore()
    pl.semaphore_signal(barrier, inc=1, device_id={"replica": other}, device_id_type=pl.DeviceIdType.MESH)

    @pl.when(row > 0)
    def _():
        pl.semaphore_signal(barrier, inc=1, device_id={"replica": me - 2}, device_id_type=pl.DeviceIdType.MESH)

    @pl.when(row < nz - 1)
    def _():
        pl.semaphore_signal(barrier, inc=1, device_id={"replica": me + 2}, device_id_type=pl.DeviceIdType.MESH)

    lax.fori_loop(1, tiles_up, lambda k, c: (load_up(k).start(), c)[1], 0)
    for p in params[:2]:
        p.start()
    mine[2 * n + 4 : 2 * n + 8, :] = jnp.zeros((4, wide), jnp.float32)
    for p in vectors:
        p.start()
    for b in range(n):
        load_down(b).start()
    for p in params[2:]:
        p.start()
    encode_a(jnp.int32(0))

    def run(z):
        poses = (z, nz - 1 - z)
        far = max(poses)
        pl.semaphore_wait(barrier, 1 + (z > 0) + (z < nz - 1))

        def beyond(d):
            return slice(z + 1, nz) if d == 0 else slice(0, z)

        def behind(d):
            return slice(0, z) if d == 0 else slice(z + 1, nz)

        def inward(d):
            return slice(z, nz) if d == 0 else slice(0, z + 1)

        def nextdev(d):
            return me + (2, -2)[d]

        def copy_a(u):
            return remote(a_s.at[u], a_r.at[u], sa.at[0], ra.at[u], other)

        def copy_c(u, d, sl):
            return remote(c_s[d].at[u, sl], c_r[d].at[u, sl], sc.at[d], rc.at[d, u], nextdev(d))

        def copy_z(u, d, sl):
            return remote(z_s[d].at[u, sl], z_r[d].at[u, sl], sz.at[d], rz.at[d, u], nextdev(d))

        def copy_y(u):
            return remote(y_s.at[u], y_r.at[u], sy.at[0], ry.at[u], other)

        def piece(ref, ss, rs, d, u):
            return remote(ref, ref, ss.at[d], rs.at[d, u], nextdev(d))

        def own_y(u, d, o):
            k, half = tile_of(u)
            return piece(gy.at[k, o, y, half], so, ro, d, u)

        def rest_y(u, d, sl):
            k, half = tile_of(u)
            return piece(gy.at[k, sl, y, half], st, rt, d, u)

        def fin_y(u):
            k, half = tile_of(u)
            ref = gy.at[k, :, y, half]
            return remote(ref, ref, sf.at[0], rf.at[0], other)

        def side_z(u, who):
            k, half = tile_of(u)
            ref = gz.at[k, z, who, half]
            return remote(ref, ref, sg.at[0], rg.at[u], other)

        def own_z(u, d, o):
            k, half = tile_of(u)
            return piece(gz.at[k, o, :, half], sp, rp, d, u)

        def rest_z(u, d, sl):
            k, half = tile_of(u)
            return piece(gz.at[k, sl, :, half], sq, rq, d, u)

        def prior(d):
            sl = behind(d)
            return z - 1 if d == 0 else z + 1, (slice(0, z - 1) if d == 0 else slice(z + 2, nz))

        def pair_y(u):
            k, half = tile_of(u)
            copy_a(u).wait_recv()
            for t in range(nz):
                at = (k, 2 * t + y, rows_y(half))
                xs[at] = xs[at] + decode(a_r[u, t], reach)

        def chain_y(u, d):
            k, half = tile_of(u)
            pos = poses[d]
            if pos > 0:
                copy_c(u, d, inward(d)).wait_recv()
            for t in range(nz)[beyond(d)]:
                value = xs[k, 2 * t + y, rows_y(half), :]
                if pos > 0:
                    value = value + decode(c_r[d][u, t], 2.0 * reach * pos)
                c_s[d][u, t] = encode(value, 2.0 * reach * (pos + 1))
            if pos < nz - 1:
                copy_c(u, d, beyond(d)).start()

        def finish(k, half, rows, count, total, put):
            at = pl.multiple_of(half * size, 8) + (0 if put is gy else part_y)

            @pl.when(k < tiles_up)
            def _():
                spot = (pl.ds(pl.multiple_of(at, 8), count), pl.ds(pl.multiple_of(k * wide, wide), wide))
                stepped, state = update(total, wu[spot], hu[spot], rate)
                ou[spot] = stepped
                qu[spot] = state
                put[k, z, y, half] = stepped.astype(jnp.bfloat16)

            @pl.when(k >= tiles_up)
            def _():
                spot = pl.ds(pl.multiple_of((k - tiles_up) * hb + at, 8), count)
                stepped, state = update(total, wd[spot, :], hd[spot, :], rate)
                od[spot, :] = stepped
                qd[spot, :] = state
                put[k, z, y, half] = stepped.astype(jnp.bfloat16)

        def close_y(u):
            k, half = tile_of(u)
            total = xs[k, me, rows_y(half), :]
            for d in range(2):
                if poses[d] > 0:
                    total = total + decode(c_r[d][u, z], 2.0 * reach * poses[d])
            finish(k, half, rows_y(half), part_y, total, gy)
            for d in range(2):
                if poses[d] < nz - 1:
                    own_y(u, d, z).start()

        def relay_y(u, d):
            pos = poses[d]
            o, sl = prior(d)
            own_y(u, d, o).wait_recv()
            if pos > 1:
                rest_y(u, d, sl).wait_recv()
            if pos < nz - 1:
                rest_y(u, d, behind(d)).start()

        def last_y(u):
            fin_y(u).start()

        def chain_z(u, d):
            k, half = tile_of(u)
            pos = poses[d]
            if pos > 0:
                copy_z(u, d, inward(d)).wait_recv()
            for t in range(nz)[beyond(d)]:
                for j in range(2):
                    value = xs[k, 2 * t + j, rows_z(half), :]
                    if pos > 0:
                        value = value + decode(z_r[d][u, t, j], reach * pos)
                    z_s[d][u, t, j] = encode(value, reach * (pos + 1))
            if pos < nz - 1:
                copy_z(u, d, beyond(d)).start()

        def cross_z(u):
            k, half = tile_of(u)
            sums = []
            for who in (1 - y, y):
                total = xs[k, 2 * z + who, rows_z(half), :]
                for d in range(2):
                    if poses[d] > 0:
                        total = total + decode(z_r[d][u, z, who], reach * poses[d])
                sums.append(total)
            y_s[u] = encode(sums[0], reach * nz)
            copy_y(u).start()
            xs[k, me, rows_z(half), :] = sums[1]

        def close_z(u):
            k, half = tile_of(u)
            copy_y(u).wait_recv()
            total = xs[k, me, rows_z(half), :] + decode(y_r[u], reach * nz)
            finish(k, half, rows_z(half), part_z, total, gz)
            side_z(u, y).start()

        def spread_z(u):
            side_z(u, 1 - y).wait_recv()
            for d in range(2):
                if poses[d] < nz - 1:
                    own_z(u, d, z).start()

        def relay_z(u, d):
            pos = poses[d]
            o, sl = prior(d)
            own_z(u, d, o).wait_recv()
            if pos > 1:
                rest_z(u, d, sl).wait_recv()
            if pos < nz - 1:
                rest_z(u, d, behind(d)).start()

        def vec_send():
            for p in vectors:
                p.wait()
            remote(mine, theirs, sv.at[0], rv.at[0], other).start()

        def vec_pair():
            remote(mine, theirs, sv.at[0], rv.at[0], other).wait_recv()
            a, b = mine[...], theirs[...]
            packs[z, 0 : 2 * n, :] = a[0 : 2 * n, :] + b[0 : 2 * n, :]
            first = y == 0
            packs[z, 2 * n : 2 * n + 8, :] = jnp.concatenate(
                [
                    jnp.where(first, a[2 * n : 2 * n + 4, :], b[2 * n : 2 * n + 4, :]),
                    jnp.where(first, b[2 * n : 2 * n + 4, :], a[2 * n : 2 * n + 4, :]),
                ],
                axis=0,
            )

        def copy_v(d, sl):
            ref = packs.at[sl]
            return remote(ref, ref, sw.at[d], rw.at[d], nextdev(d))

        def through(d):
            return slice(0, z + 1) if d == 0 else slice(z, nz)

        def vec_chain(d):
            if poses[d] > 0:
                copy_v(d, behind(d)).wait_recv()
            if poses[d] < nz - 1:
                copy_v(d, through(d)).start()

        def vec_close():
            total = packs[0, 0 : 2 * n, :]
            for t in range(1, nz):
                total = total + packs[t, 0 : 2 * n, :]
            for t in range(nz):
                held = packs[t, 2 * n : 2 * n + 8, :]
                for j in range(2):
                    for i in range(4):
                        at = i * n + 2 * t + j
                        hold_s[at : at + 1, :] = held[4 * j + i : 4 * j + i + 1, :]
            stepped, state = update(total, hold_s[0 : 2 * n, :], hold_s[2 * n : 4 * n, :], rate)
            cn[...] = stepped[0:n].astype(jnp.bfloat16)
            cb[...] = stepped[n : 2 * n].astype(jnp.bfloat16)
            step_s[...] = stepped
            state_s[...] = state

        at_sum = LAG_PAIR
        at_spread = LAG_PAIR + LAG_SUM * (nz - 1)
        side_sum = LAG_SUM * far
        side_spread = LAG_SUM * (nz - 1) + 2 * LAG_SIDE
        plan = [(0, lambda u: copy_a(u).start())]
        for d in range(2):
            if poses[d] > 0:
                plan.append((at_spread + LAG_GATHER * poses[d], functools.partial(relay_y, d=d)))
        plan.append((at_spread + LAG_GATHER * far, last_y))
        for d in range(2):
            if poses[d] > 0:
                plan.append((side_spread + LAG_GATHER * poses[d], functools.partial(relay_z, d=d)))
        plan.append((side_sum + 2 * LAG_SIDE, spread_z))
        for d in range(2):
            plan.append((LAG_SUM * poses[d], functools.partial(chain_z, d=d)))
        plan.append((side_sum, cross_z))
        plan.append((at_sum, pair_y))
        for d in range(2):
            plan.append((at_sum + LAG_SUM * poses[d], functools.partial(chain_y, d=d)))
        plan.append((at_sum + LAG_SUM * far, close_y))
        plan.append((side_sum + LAG_SIDE, close_z))
        plan.append((-1, encode_a))
        slots = units + max(lag for lag, _ in plan)
        vec_at = 2 + LAG_VECTOR
        extra = [(2, vec_send), (vec_at, vec_pair)]
        extra += [(vec_at + LAG_VECTOR * poses[d], functools.partial(vec_chain, d)) for d in range(2)]
        extra.append((vec_at + LAG_VECTOR * nz, vec_close))
        first_close = min(at_sum + LAG_SUM * far, side_sum + LAG_SIDE)

        def slot(s, carry):
            @pl.when(s == first_close)
            def _():
                for p in params:
                    p.wait()

            for lag, task in plan:
                u = s - lag

                @pl.when(jnp.logical_and(u >= 0, u < units))
                def _():
                    task(u)

            for when, step in extra:
                pl.when(s == when)(step)

            return carry

        lax.fori_loop(0, slots, slot, 0)

        remote(a_s, a_r, sa.at[0], ra.at[0], other).wait_send()
        for d in range(2):
            if poses[d] < nz - 1:
                copy_c(slice(None), d, beyond(d)).wait_send()
                copy_z(slice(None), d, beyond(d)).wait_send()
                ref = gy.at[:, z, y]
                remote(ref, ref, so.at[d], ro.at[d, 0], other).wait_send()
                ref = gz.at[:, z]
                remote(ref, ref, sp.at[d], rp.at[d, 0], other).wait_send()
                if poses[d] > 0:
                    ref = gy.at[:, behind(d), y]
                    remote(ref, ref, st.at[d], rt.at[d, 0], other).wait_send()
                    ref = gz.at[:, behind(d)]
                    remote(ref, ref, sq.at[d], rq.at[d, 0], other).wait_send()
                copy_v(d, through(d)).wait_send()
        remote(y_s, y_r, sy.at[0], ry.at[0], other).wait_send()
        ref = gz.at[:, z, y]
        remote(ref, ref, sg.at[0], rg.at[0], other).wait_send()
        remote(mine, theirs, sv.at[0], rv.at[0], other).wait_send()
        ref = gy.at[:, :, y]
        remote(ref, ref, sf.at[0], rf.at[0], other).wait_send()
        ref = gy.at[:, :, 1 - y]
        remote(ref, ref, sf.at[0], rf.at[0], other).wait_recv()

    for z in range(nz):
        pl.when(row == z)(functools.partial(run, z))


def leave(
    n, gy, gz, ou, od, qu, qd, cn, cb, step_s, state_s,
    cu, cd, tu, td, vu, vd, xcn, xcb, tn, tb, vn, vb, sem,
):
    me = lax.axis_index("replica")
    tiles, nz, _, halves, part_y, wide = gy.shape
    tiles_up = cu.shape[4] // wide
    size = cu.shape[3]
    pairs = []
    for ref, lo, hi in ((gy, 0, part_y), (gz, part_y, size)):
        for k in range(tiles_up):
            pairs.append((ref.at[k], cu.at[:, :, :, lo:hi, k * wide : (k + 1) * wide]))
        for b in range(n):
            pairs.append((ref.at[tiles_up:tiles, b // 2, b % 2], cd.at[:, :, lo:hi, b * wide : (b + 1) * wide]))
    pairs += [(ou, tu), (od, td), (qu, vu), (qd, vd), (cn, xcn), (cb, xcb)]
    pairs += [(step_s.at[pl.ds(me, 1), :], tn), (step_s.at[pl.ds(me + n, 1), :], tb)]
    pairs += [(state_s.at[pl.ds(me, 1), :], vn), (state_s.at[pl.ds(me + n, 1), :], vb)]
    copies = [pltpu.make_async_copy(a, b, sem.at[i]) for i, (a, b) in enumerate(pairs)]
    for c in copies:
        c.start()
    for c in copies:
        c.wait()


def fused(
    n, partial_up, partial_down, partial_norm, partial_bias, master_up, master_down,
    master_norm, master_bias, memory_up, memory_down, memory_norm, memory_bias,
):
    H = HALVES
    nz = n // 2
    hb, w = master_up.shape
    rows, wide = master_down.shape
    size, part_y, part_z = shares(hb)
    tiles_up, tiles_down = w // wide, rows // hb
    tiles = tiles_up + tiles_down
    units = tiles * H
    f32, b16 = jnp.float32, jnp.bfloat16
    line = lambda a: a.reshape(1, -1)
    operands = (
        partial_up[0].reshape(n, hb, w), partial_down[0].reshape(tiles_down, hb, n * wide),
        master_up, master_down, memory_up, memory_down,
        partial_norm.reshape(n, -1), partial_bias.reshape(n, -1),
        line(master_norm), line(master_bias), line(memory_norm), line(memory_bias),
    )
    S = jax.ShapeDtypeStruct
    shapes = (
        S((nz, 2, H, size, w), b16), S((tiles_down, H, size, n * wide), b16),
        S((hb, w), f32), S((rows, wide), f32), S((hb, w), f32), S((rows, wide), f32),
        S((n, wide), b16), S((n, wide), b16),
        S((1, wide), f32), S((1, wide), f32), S((1, wide), f32), S((1, wide), f32),
    )
    hbm = pl.BlockSpec(memory_space=pltpu.HBM)
    vm = pl.BlockSpec(memory_space=pltpu.VMEM)
    D = pltpu.SemaphoreType.DMA
    V = pltpu.VMEM
    one, two, each, both = D((1,)), D((2,)), D((units,)), D((2, units))
    held = pl.pallas_call(
        functools.partial(kernel, n),
        out_shape=(
            S((tiles, nz, 2, H, part_y, wide), b16), S((tiles, nz, 2, H, part_z, wide), b16),
            S((hb, w), f32), S((rows, wide), f32), S((hb, w), f32), S((rows, wide), f32),
            S((n, wide), b16), S((n, wide), b16), S((2 * n, wide), f32), S((2 * n, wide), f32),
        ),
        in_specs=[hbm] * 12,
        out_specs=[vm] * 10,
        scratch_shapes=[
            V((tiles, n, hb, wide), f32),
            V((hb, w), f32), V((rows, wide), f32), V((hb, w), f32), V((rows, wide), f32),
            *[V((units, nz, part_y, wide), b16)] * 6,
            *[V((units, nz, 2, part_z, wide), b16)] * 4,
            *[V((units, part_z, wide), b16)] * 2,
            V((2 * n + 8, wide), f32), V((2 * n + 8, wide), f32), V((nz, 2 * n + 8, wide), f32), V((4 * n, wide), f32),
            D((tiles_up,)), D((n,)), D((4,)), D((6,)),
            one, each, two, both, two, both, one, each, two, both, two, both,
            one, one, one, each, two, both, two, both, one, one, two, two,
        ],
        compiler_params=pltpu.CompilerParams(
            collective_id=0, has_side_effects=True, vmem_limit_bytes=28 * 1024 * 1024
        ),
    )(*[pltpu.with_memory_space_constraint(a, pltpu.HBM) for a in operands])
    cu, cd, tu, td, vu, vd, cn, cb, tn, tb, vn, vb = pl.pallas_call(
        functools.partial(leave, n),
        out_shape=shapes,
        in_specs=[vm] * 10,
        out_specs=[hbm] * 12,
        scratch_shapes=[D((2 * (tiles_up + n) + 10,))],
        compiler_params=pltpu.CompilerParams(vmem_limit_bytes=4 * 1024 * 1024),
    )(*held)
    flat = lambda a: a.reshape(-1)
    return (
        cu.reshape(n * hb, w), cd.reshape(rows, n * wide), flat(cn), flat(cb),
        tu, td, flat(tn), flat(tb), vu, vd, flat(vn), flat(vb),
    )


def on_device(*args):
    n = lax.axis_size("replica")
    (hb, w), (rows, wide) = args[4].shape, args[5].shape
    fits = n % 8 == 0 and n < 16 and wide == 128 and args[6].shape[0] == wide and args[7].shape[0] == wide
    fits = fits and hb % (32 * HALVES) == 0 and rows % hb == 0 and w % wide == 0
    return fused(n, *args) if fits else plain(*args)


def solution(mesh):
    in_specs = (
        P("replica", None, "model"),
        P("replica", "model", None),
        P("replica", None),
        P("replica", None),
        P("replica", "model"),
        P("model", "replica"),
        P("replica"),
        P("replica"),
        P("replica", "model"),
        P("model", "replica"),
        P("replica"),
        P("replica"),
    )
    out_specs = (
        P(None, "model"),
        P("model", None),
        P(),
        P(),
        P("replica", "model"),
        P("model", "replica"),
        P("replica"),
        P("replica"),
        P("replica", "model"),
        P("model", "replica"),
        P("replica"),
        P("replica"),
    )
    return jax.shard_map(
        on_device, mesh=mesh, in_specs=in_specs, out_specs=out_specs, check_vma=False
    )
```

```python
import functools
import math

import jax
import jax.numpy as jnp
from jax import lax
from jax.experimental import pallas as pl
from jax.experimental.pallas import tpu as pltpu
from jax.sharding import PartitionSpec as P

learn_rate = 0.05
hold_rate = 0.9


def plain(
    partial_up,
    partial_down,
    partial_norm,
    partial_bias,
    master_up,
    master_down,
    master_norm,
    master_bias,
    memory_up,
    memory_down,
    memory_norm,
    memory_bias,
):
    mean_up, mean_down = (
        lax.psum_scatter(partial_up[0], "replica", scatter_dimension=0, tiled=True),
        lax.psum_scatter(partial_down[0], "replica", scatter_dimension=1, tiled=True),
    )
    whole_norm, whole_bias = lax.psum((partial_norm[0], partial_bias[0]), "replica")
    place = lax.axis_index("replica")
    mean_norm = lax.dynamic_slice_in_dim(
        whole_norm, place * master_norm.shape[0], master_norm.shape[0]
    )
    mean_bias = lax.dynamic_slice_in_dim(
        whole_bias, place * master_bias.shape[0], master_bias.shape[0]
    )
    mean_rate = lax.axis_size("replica") ** (-0.5)
    mean_up = mean_up * mean_rate
    mean_down = mean_down * mean_rate
    mean_norm = mean_norm * mean_rate
    mean_bias = mean_bias * mean_rate
    state_new_up = hold_rate * memory_up + (1.0 - hold_rate) * mean_up * mean_up
    stepped_up = master_up - learn_rate * mean_up * lax.rsqrt(state_new_up + 1e-06)
    state_new_down = hold_rate * memory_down + (1.0 - hold_rate) * mean_down * mean_down
    stepped_down = master_down - learn_rate * mean_down * lax.rsqrt(state_new_down + 1e-06)
    state_new_norm = hold_rate * memory_norm + (1.0 - hold_rate) * mean_norm * mean_norm
    stepped_norm = master_norm - learn_rate * mean_norm * lax.rsqrt(state_new_norm + 1e-06)
    state_new_bias = hold_rate * memory_bias + (1.0 - hold_rate) * mean_bias * mean_bias
    stepped_bias = master_bias - learn_rate * mean_bias * lax.rsqrt(state_new_bias + 1e-06)
    compute_up, compute_down, compute_norm, compute_bias = (
        lax.all_gather(stepped_up.astype(jnp.bfloat16), "replica", axis=0, tiled=True),
        lax.all_gather(stepped_down.astype(jnp.bfloat16), "replica", axis=1, tiled=True),
        lax.all_gather(stepped_norm.astype(jnp.bfloat16), "replica", axis=0, tiled=True),
        lax.all_gather(stepped_bias.astype(jnp.bfloat16), "replica", axis=0, tiled=True),
    )
    return (
        compute_up,
        compute_down,
        compute_norm,
        compute_bias,
        stepped_up,
        stepped_down,
        stepped_norm,
        stepped_bias,
        state_new_up,
        state_new_down,
        state_new_norm,
        state_new_bias,
    )


SHARE = 3 / 4
SPAN = 124.0
POWER = 49
STEEP = 2.0 ** (2.0 * SPAN / POWER) - 1.0
LOW = 2.0 ** (-SPAN / POWER)
LAG_PAIR = 7
SUM_Y = (0, 4, 7, 10)
SUM_Z = (0, 4, 7, 11)
RELAY_Y = (0, 5, 8, 16)
RELAY_Z = (0, 21, 29, 48)
LAG_CLOSE = 4
LAG_SPREAD = 4
LAG_LAST = 2
LAG_VECTOR = 4
LAG_OWN = 4
LAG_NEAR = 9
HEAD_START = 2000
HOLD_Y = (1, 1, 0)
HOLD_Z = (14, 25, 0)
ORDER = ('rz', 'py', 'cy', 'a', 'cly', 'cz', 'spz', 'oz', 'clz', 'wy', 'oy', 'xz', 'f1', 'f', 'ry', 'ea')


def encode(x, reach):
    q = x * (LOW * STEEP / reach) + jnp.where(x < 0.0, -LOW, LOW)
    q2 = q * q
    q3 = q2 * q
    q6 = q3 * q3
    q12 = q6 * q6
    q24 = q12 * q12
    q48 = q24 * q24
    return (q48 * q).astype(jnp.bfloat16)


def decode(code, reach):
    y = code.astype(jnp.float32)
    grown = jnp.exp2(jnp.log(jnp.abs(y)) * (1.0 / (math.log(2.0) * POWER)))
    scale = reach / (LOW * STEEP)
    return (grown - LOW) * jnp.where(y < 0.0, -scale, scale)


def update(total, master, memory, rate):
    mean = total * rate
    state = hold_rate * memory + (1.0 - hold_rate) * mean * mean
    return master - learn_rate * mean * lax.rsqrt(state + 1e-06), state


def shares(hb):
    part_y = int(hb * SHARE) // 8 * 8
    cut_y, cut_z = -(-part_y // 32) * 16, (hb - part_y) // 32 * 16
    return (0, cut_y, part_y), (0, cut_z, hb - part_y)


def kernel(
    n,
    pu, pd, mu, md, su, sd, pn, pb, mn, mb, sn, sb,
    gy, gz, ou, od, qu, qd, cn, cb, step_s, state_s,
    xs, wu, wd, hu, hd,
    a_s, a_r, c_s0, c_s1, c_r0, c_r1, z_s0, z_s1, z_r0, z_r1, y_s, y_r,
    mine, theirs, packs, hold_s,
    sem_up, sem_down, sem_par, sem_vec,
    sa, ra, sc, rc, sz, rz, sy, ry, so, ro, st, rt, sf, rf, sg, rg, sp, rp, sq, rq, sv, rv, sw, rw,
):
    nz = n // 2
    tiles, _, hb, wide = xs.shape
    cuts_y, cuts_z = shares(hb)
    tiles_up = pu.shape[2] // wide
    me = lax.axis_index("replica")
    y = lax.rem(me, 2)
    row = lax.div(me, 2)
    other = me + 1 - 2 * y
    rate = n ** (-0.5)
    reach = n / 2.0
    c_s, c_r, z_s, z_r = (c_s0, c_s1), (c_r0, c_r1), (z_s0, z_s1), (z_r0, z_r1)

    def remote(src, dst, ss, rs, who):
        return pltpu.make_async_remote_copy(
            src_ref=src, dst_ref=dst, send_sem=ss, recv_sem=rs,
            device_id={"replica": who}, device_id_type=pl.DeviceIdType.MESH,
        )

    def load_up(k):
        lanes = pl.ds(pl.multiple_of(k * wide, wide), wide)
        return pltpu.make_async_copy(pu.at[:, :, lanes], xs.at[k], sem_up.at[k])

    def load_down(b):
        return pltpu.make_async_copy(
            pd.at[:, :, b * wide : (b + 1) * wide], xs.at[tiles_up:tiles, b], sem_down.at[b]
        )

    params = [
        pltpu.make_async_copy(a, b, sem_par.at[i])
        for i, (a, b) in enumerate(((mu, wu), (su, hu), (md, wd), (sd, hd)))
    ]
    vectors = [
        pltpu.make_async_copy(a, mine.at[at : at + a.shape[0], :], sem_vec.at[i])
        for i, (a, at) in enumerate(
            ((pn, 0), (pb, n), (mn, 2 * n), (mb, 2 * n + 1), (sn, 2 * n + 2), (sb, 2 * n + 3))
        )
    ]

    def rows_y(half):
        return slice(cuts_y[half], cuts_y[half + 1])

    def rows_z(half):
        return slice(cuts_z[half], cuts_z[half + 1])

    def rows_zx(half):
        return slice(cuts_y[2] + cuts_z[half], cuts_y[2] + cuts_z[half + 1])

    def encode_a(k, half):
        if half == 0:

            @pl.when(k < tiles_up)
            def _():
                load_up(k).wait()

            @pl.when(k == tiles_up)
            def _():
                for b in range(n):
                    load_down(b).wait()

        for t in range(nz):
            a_s[k, t, rows_y(half)] = encode(xs[k, 2 * t + 1 - y, rows_y(half), :], reach)

    load_up(0).start()
    barrier = pltpu.get_barrier_semaphore()
    pl.semaphore_signal(barrier, inc=1, device_id={"replica": other}, device_id_type=pl.DeviceIdType.MESH)

    @pl.when(row > 0)
    def _():
        pl.semaphore_signal(barrier, inc=1, device_id={"replica": me - 2}, device_id_type=pl.DeviceIdType.MESH)

    @pl.when(row < nz - 1)
    def _():
        pl.semaphore_signal(barrier, inc=1, device_id={"replica": me + 2}, device_id_type=pl.DeviceIdType.MESH)

    lax.fori_loop(1, tiles_up, lambda k, c: (load_up(k).start(), c)[1], 0)
    for p in params[:2]:
        p.start()
    mine[2 * n + 4 : 2 * n + 8, :] = jnp.zeros((4, wide), jnp.float32)
    for p in vectors:
        p.start()
    for b in range(n):
        load_down(b).start()
    for p in params[2:]:
        p.start()
    encode_a(jnp.int32(0), 0)

    def run(z):
        poses = (z, nz - 1 - z)
        far = max(poses)
        pl.semaphore_wait(barrier, 1 + (z > 0) + (z < nz - 1))
        pl.when(lax.rem(lax.axis_index("model"), 2) == 1)(lambda: pl.delay(HEAD_START))

        def beyond(d):
            return slice(z + 1, nz) if d == 0 else slice(0, z)

        def behind(d):
            return slice(0, z) if d == 0 else slice(z + 1, nz)

        def inward(d):
            return slice(z, nz) if d == 0 else slice(0, z + 1)

        def nextdev(d):
            return me + (2, -2)[d]

        def copy_a(k, half):
            r = rows_y(half)
            return remote(a_s.at[k, :, r], a_r.at[k, :, r], sa.at[0], ra.at[2 * k + half], other)

        def copy_c(k, half, d, sl):
            r = rows_y(half)
            return remote(c_s[d].at[k, sl, r], c_r[d].at[k, sl, r], sc.at[d], rc.at[d, 2 * k + half], nextdev(d))

        def copy_z(k, half, d, sl):
            r = rows_z(half)
            return remote(z_s[d].at[k, sl, :, r], z_r[d].at[k, sl, :, r], sz.at[d], rz.at[d, 2 * k + half], nextdev(d))

        def copy_y(k, half):
            r = rows_z(half)
            return remote(y_s.at[k, r], y_r.at[k, r], sy.at[0], ry.at[2 * k + half], other)

        def piece(ref, ss, rs, k, half, d):
            return remote(ref, ref, ss.at[d], rs.at[d, 2 * k + half], nextdev(d))

        def own_y(k, half, d, o):
            return piece(gy.at[k, o, y, rows_y(half)], so, ro, k, half, d)

        def rest_y(k, half, d, sl):
            return piece(gy.at[k, sl, y, rows_y(half)], st, rt, k, half, d)

        def fin_y(k, half, lo):
            ref = gy.at[k, lo : lo + 2, y, rows_y(half)]
            return remote(ref, ref, sf.at[0], rf.at[0], other)

        def side_z(k, half, who):
            ref = gz.at[k, z, who, rows_z(half)]
            return remote(ref, ref, sg.at[0], rg.at[2 * k + half], other)

        def own_z(k, half, d, o):
            return piece(gz.at[k, o, :, rows_z(half)], sp, rp, k, half, d)

        def rest_z(k, half, d, sl):
            return piece(gz.at[k, sl, :, rows_z(half)], sq, rq, k, half, d)

        def prior(d):
            return (z - 1, slice(0, z - 1)) if d == 0 else (z + 1, slice(z + 2, nz))

        def pair_y(k, half):
            r = rows_y(half)
            copy_a(k, half).wait_recv()
            for t in range(nz):
                at = (k, 2 * t + y, r)
                xs[at] = xs[at] + decode(a_r[k, t, r], reach)

        def chain_y(k, half, d):
            r = rows_y(half)
            pos = poses[d]
            if pos > 0:
                copy_c(k, half, d, inward(d)).wait_recv()
            for t in range(nz)[beyond(d)]:
                value = xs[k, 2 * t + y, r, :]
                if pos > 0:
                    value = value + decode(c_r[d][k, t, r], 2.0 * reach * pos)
                c_s[d][k, t, r] = encode(value, 2.0 * reach * (pos + 1))
            if pos < nz - 1:
                copy_c(k, half, d, beyond(d)).start()

        def finish(k, r, total, put, place):
            @pl.when(k < tiles_up)
            def _():
                spot = (r, pl.ds(pl.multiple_of(k * wide, wide), wide))
                stepped, state = update(total, wu[spot], hu[spot], rate)
                ou[spot] = stepped
                qu[spot] = state
                put[k, z, y, place] = stepped.astype(jnp.bfloat16)

            @pl.when(k >= tiles_up)
            def _():
                spot = pl.ds(pl.multiple_of((k - tiles_up) * hb + r.start, 8), r.stop - r.start)
                stepped, state = update(total, wd[spot, :], hd[spot, :], rate)
                od[spot, :] = stepped
                qd[spot, :] = state
                put[k, z, y, place] = stepped.astype(jnp.bfloat16)

        def close_y(k, half):
            r = rows_y(half)
            total = xs[k, me, r, :]
            for d in range(2):
                if poses[d] > 0:
                    total = total + decode(c_r[d][k, z, r], 2.0 * reach * poses[d])
            finish(k, r, total, gy, r)

        def send_y(k, half, d):
            own_y(k, half, d, z).start()

        def relay_y(k, half, d):
            pos = poses[d]
            sl = prior(d)[1]
            if pos > 1:
                rest_y(k, half, d, sl).wait_recv()
            if pos < nz - 1:
                rest_y(k, half, d, behind(d)).start()

        def heard_y(k, half, d):
            own_y(k, half, d, prior(d)[0]).wait_recv()

        def near_y(k, half):
            fin_y(k, half, z // 2 * 2).start()

        def last_y(k, half):
            for lo in range(0, nz, 2):
                if lo != z // 2 * 2:
                    fin_y(k, half, lo).start()

        def chain_z(k, half, d):
            r = rows_z(half)
            pos = poses[d]
            if pos > 0:
                copy_z(k, half, d, inward(d)).wait_recv()
            for t in range(nz)[beyond(d)]:
                for j in range(2):
                    value = xs[k, 2 * t + j, rows_zx(half), :]
                    if pos > 0:
                        value = value + decode(z_r[d][k, t, j, r], reach * pos)
                    z_s[d][k, t, j, r] = encode(value, reach * (pos + 1))
            if pos < nz - 1:
                copy_z(k, half, d, beyond(d)).start()

        def cross_z(k, half):
            r = rows_z(half)
            sums = []
            for who in (1 - y, y):
                total = xs[k, 2 * z + who, rows_zx(half), :]
                for d in range(2):
                    if poses[d] > 0:
                        total = total + decode(z_r[d][k, z, who, r], reach * poses[d])
                sums.append(total)
            y_s[k, r] = encode(sums[0], reach * nz)
            copy_y(k, half).start()
            xs[k, me, rows_zx(half), :] = sums[1]

        def close_z(k, half):
            r = rows_z(half)
            copy_y(k, half).wait_recv()
            total = xs[k, me, rows_zx(half), :] + decode(y_r[k, r], reach * nz)
            finish(k, rows_zx(half), total, gz, r)
            side_z(k, half, y).start()

        def spread_z(k, half):
            side_z(k, half, 1 - y).wait_recv()

        def send_z(k, half, d):
            own_z(k, half, d, z).start()

        def relay_z(k, half, d):
            pos = poses[d]
            o, sl = prior(d)
            own_z(k, half, d, o).wait_recv()
            if pos > 1:
                rest_z(k, half, d, sl).wait_recv()
            if pos < nz - 1:
                rest_z(k, half, d, behind(d)).start()

        def vec_send():
            for p in vectors:
                p.wait()
            remote(mine, theirs, sv.at[0], rv.at[0], other).start()

        def vec_pair():
            remote(mine, theirs, sv.at[0], rv.at[0], other).wait_recv()
            a, b = mine[...], theirs[...]
            packs[z, 0 : 2 * n, :] = a[0 : 2 * n, :] + b[0 : 2 * n, :]
            first = y == 0
            packs[z, 2 * n : 2 * n + 8, :] = jnp.concatenate(
                [
                    jnp.where(first, a[2 * n : 2 * n + 4, :], b[2 * n : 2 * n + 4, :]),
                    jnp.where(first, b[2 * n : 2 * n + 4, :], a[2 * n : 2 * n + 4, :]),
                ],
                axis=0,
            )

        def copy_v(d, sl):
            ref = packs.at[sl]
            return remote(ref, ref, sw.at[d], rw.at[d], nextdev(d))

        def through(d):
            return slice(0, z + 1) if d == 0 else slice(z, nz)

        def vec_chain(d):
            if poses[d] > 0:
                copy_v(d, behind(d)).wait_recv()
            if poses[d] < nz - 1:
                copy_v(d, through(d)).start()

        def vec_close():
            total = packs[0, 0 : 2 * n, :]
            for t in range(1, nz):
                total = total + packs[t, 0 : 2 * n, :]
            for t in range(nz):
                held = packs[t, 2 * n : 2 * n + 8, :]
                for j in range(2):
                    for i in range(4):
                        at = i * n + 2 * t + j
                        hold_s[at : at + 1, :] = held[4 * j + i : 4 * j + i + 1, :]
            stepped, state = update(total, hold_s[0 : 2 * n, :], hold_s[2 * n : 4 * n, :], rate)
            cn[...] = stepped[0:n].astype(jnp.bfloat16)
            cb[...] = stepped[n : 2 * n].astype(jnp.bfloat16)
            step_s[...] = stepped
            state_s[...] = state

        at_spread = LAG_PAIR + SUM_Y[nz - 1]
        at_close = LAG_PAIR + SUM_Y[far]
        side_sum = SUM_Z[far]
        side_close = side_sum + LAG_CLOSE
        side_open = side_close + LAG_SPREAD
        side_spread = SUM_Z[nz - 1] + LAG_CLOSE + LAG_SPREAD
        heard = {}
        for d in range(2):
            before = poses[d] - 1
            if before >= 0:
                heard[d] = LAG_PAIR + SUM_Y[max(before, nz - 1 - before)] + HOLD_Y[before] + LAG_OWN
        at_near = max(at_close, heard[1 - z % 2]) + LAG_NEAR
        tasks = {
            "wy": [(heard[d], functools.partial(heard_y, d=d)) for d in heard],
            "f1": [(at_near, near_y)],
            "a": [(0, lambda k, half: copy_a(k, half).start())],
            "ea": [(-1, encode_a)],
            "py": [(LAG_PAIR, pair_y)],
            "cy": [(LAG_PAIR + SUM_Y[poses[d]], functools.partial(chain_y, d=d)) for d in range(2)],
            "cly": [(at_close, close_y)],
            "oy": [(at_close + HOLD_Y[poses[d]], functools.partial(send_y, d=d)) for d in range(2) if poses[d] < nz - 1],
            "oz": [(side_open + HOLD_Z[poses[d]], functools.partial(send_z, d=d)) for d in range(2) if poses[d] < nz - 1],
            "ry": [(at_spread + RELAY_Y[poses[d]], functools.partial(relay_y, d=d)) for d in range(2) if poses[d] > 0],
            "f": [(at_spread + RELAY_Y[far] + LAG_LAST, last_y)],
            "cz": [(SUM_Z[poses[d]], functools.partial(chain_z, d=d)) for d in range(2)],
            "xz": [(side_sum, cross_z)],
            "clz": [(side_close, close_z)],
            "spz": [(side_open, spread_z)],
            "rz": [(side_spread + RELAY_Z[poses[d]], functools.partial(relay_z, d=d)) for d in range(2) if poses[d] > 0],
        }
        plan = [step for name in ORDER for step in tasks[name]]
        slots = 2 * tiles + max(lag for lag, _ in plan)
        vec_at = 2 + LAG_VECTOR
        extra = [(2, vec_send), (vec_at, vec_pair)]
        extra += [(vec_at + LAG_VECTOR * poses[d], functools.partial(vec_chain, d)) for d in range(2)]
        extra.append((vec_at + LAG_VECTOR * nz, vec_close))
        extra.append((min(at_close, side_close), lambda: [p.wait() for p in params] and None))

        def slot(v, carry):
            for i in range(2):
                for when, step in extra:
                    if when % 2 == i:
                        pl.when(v == when // 2)(step)

                for lag, task in plan:
                    half = (i - lag) % 2
                    k = v + (i - lag - half) // 2
                    pl.when(jnp.logical_and(k >= 0, k < tiles))(functools.partial(task, k, half))

            return carry

        lax.fori_loop(0, (slots + 1) // 2, slot, 0)

        remote(a_s, a_r, sa.at[0], ra.at[0], other).wait_send()
        for d in range(2):
            if poses[d] < nz - 1:
                remote(c_s[d].at[:, beyond(d)], c_r[d].at[:, beyond(d)], sc.at[d], rc.at[d, 0], other).wait_send()
                remote(z_s[d].at[:, beyond(d)], z_r[d].at[:, beyond(d)], sz.at[d], rz.at[d, 0], other).wait_send()
                ref = gy.at[:, z, y]
                remote(ref, ref, so.at[d], ro.at[d, 0], other).wait_send()
                ref = gz.at[:, z]
                remote(ref, ref, sp.at[d], rp.at[d, 0], other).wait_send()
                if poses[d] > 0:
                    ref = gy.at[:, behind(d), y]
                    remote(ref, ref, st.at[d], rt.at[d, 0], other).wait_send()
                    ref = gz.at[:, behind(d)]
                    remote(ref, ref, sq.at[d], rq.at[d, 0], other).wait_send()
                copy_v(d, through(d)).wait_send()
        remote(y_s, y_r, sy.at[0], ry.at[0], other).wait_send()
        ref = gz.at[:, z, y]
        remote(ref, ref, sg.at[0], rg.at[0], other).wait_send()
        remote(mine, theirs, sv.at[0], rv.at[0], other).wait_send()
        ref = gy.at[:, :, y]
        remote(ref, ref, sf.at[0], rf.at[0], other).wait_send()
        ref = gy.at[:, :, 1 - y]
        remote(ref, ref, sf.at[0], rf.at[0], other).wait_recv()

    for z in range(nz):
        pl.when(row == z)(functools.partial(run, z))


def leave(
    n, gy, gz, ou, od, qu, qd, cn, cb, step_s, state_s,
    cu, cd, tu, td, vu, vd, xcn, xcb, tn, tb, vn, vb, sem,
):
    me = lax.axis_index("replica")
    tiles, nz, _, part_y, wide = gy.shape
    tiles_up = cu.shape[3] // wide
    size = cu.shape[2]
    pairs = []
    for ref, lo, hi in ((gy, 0, part_y), (gz, part_y, size)):
        for k in range(tiles_up):
            pairs.append((ref.at[k], cu.at[:, :, lo:hi, k * wide : (k + 1) * wide]))
        for b in range(n):
            pairs.append((ref.at[tiles_up:tiles, b // 2, b % 2], cd.at[:, lo:hi, b * wide : (b + 1) * wide]))
    pairs += [(ou, tu), (od, td), (qu, vu), (qd, vd), (cn, xcn), (cb, xcb)]
    pairs += [(step_s.at[pl.ds(me, 1), :], tn), (step_s.at[pl.ds(me + n, 1), :], tb)]
    pairs += [(state_s.at[pl.ds(me, 1), :], vn), (state_s.at[pl.ds(me + n, 1), :], vb)]
    copies = [pltpu.make_async_copy(a, b, sem.at[i]) for i, (a, b) in enumerate(pairs)]
    for c in copies:
        c.start()
    for c in copies:
        c.wait()


def fused(
    n, partial_up, partial_down, partial_norm, partial_bias, master_up, master_down,
    master_norm, master_bias, memory_up, memory_down, memory_norm, memory_bias,
):
    nz = n // 2
    hb, w = master_up.shape
    rows, wide = master_down.shape
    cuts_y, cuts_z = shares(hb)
    part_y, part_z = cuts_y[2], cuts_z[2]
    tiles_up, tiles_down = w // wide, rows // hb
    tiles = tiles_up + tiles_down
    units = tiles * 2
    f32, b16 = jnp.float32, jnp.bfloat16
    line = lambda a: a.reshape(1, -1)
    operands = (
        partial_up[0].reshape(n, hb, w), partial_down[0].reshape(tiles_down, hb, n * wide),
        master_up, master_down, memory_up, memory_down,
        partial_norm.reshape(n, -1), partial_bias.reshape(n, -1),
        line(master_norm), line(master_bias), line(memory_norm), line(memory_bias),
    )
    S = jax.ShapeDtypeStruct
    shapes = (
        S((nz, 2, hb, w), b16), S((tiles_down, hb, n * wide), b16),
        S((hb, w), f32), S((rows, wide), f32), S((hb, w), f32), S((rows, wide), f32),
        S((n, wide), b16), S((n, wide), b16),
        S((1, wide), f32), S((1, wide), f32), S((1, wide), f32), S((1, wide), f32),
    )
    hbm = pl.BlockSpec(memory_space=pltpu.HBM)
    vm = pl.BlockSpec(memory_space=pltpu.VMEM)
    D = pltpu.SemaphoreType.DMA
    V = pltpu.VMEM
    one, two, each, both = D((1,)), D((2,)), D((units,)), D((2, units))
    held = pl.pallas_call(
        functools.partial(kernel, n),
        out_shape=(
            S((tiles, nz, 2, part_y, wide), b16), S((tiles, nz, 2, part_z, wide), b16),
            S((hb, w), f32), S((rows, wide), f32), S((hb, w), f32), S((rows, wide), f32),
            S((n, wide), b16), S((n, wide), b16), S((2 * n, wide), f32), S((2 * n, wide), f32),
        ),
        in_specs=[hbm] * 12,
        out_specs=[vm] * 10,
        scratch_shapes=[
            V((tiles, n, hb, wide), f32),
            V((hb, w), f32), V((rows, wide), f32), V((hb, w), f32), V((rows, wide), f32),
            *[V((tiles, nz, part_y, wide), b16)] * 6,
            *[V((tiles, nz, 2, part_z, wide), b16)] * 4,
            *[V((tiles, part_z, wide), b16)] * 2,
            V((2 * n + 8, wide), f32), V((2 * n + 8, wide), f32), V((nz, 2 * n + 8, wide), f32), V((4 * n, wide), f32),
            D((tiles_up,)), D((n,)), D((4,)), D((6,)),
            one, each, two, both, two, both, one, each, two, both, two, both,
            one, one, one, each, two, both, two, both, one, one, two, two,
        ],
        compiler_params=pltpu.CompilerParams(
            collective_id=0, has_side_effects=True, vmem_limit_bytes=28 * 1024 * 1024
        ),
    )(*[pltpu.with_memory_space_constraint(a, pltpu.HBM) for a in operands])
    cu, cd, tu, td, vu, vd, cn, cb, tn, tb, vn, vb = pl.pallas_call(
        functools.partial(leave, n),
        out_shape=shapes,
        in_specs=[vm] * 10,
        out_specs=[hbm] * 12,
        scratch_shapes=[D((2 * (tiles_up + n) + 10,))],
        compiler_params=pltpu.CompilerParams(vmem_limit_bytes=4 * 1024 * 1024),
    )(*held)
    flat = lambda a: a.reshape(-1)
    return (
        cu.reshape(n * hb, w), cd.reshape(rows, n * wide), flat(cn), flat(cb),
        tu, td, flat(tn), flat(tb), vu, vd, flat(vn), flat(vb),
    )


def on_device(*args):
    n = lax.axis_size("replica")
    (hb, w), (rows, wide) = args[4].shape, args[5].shape
    fits = n % 8 == 0 and n < 16 and wide == 128 and args[6].shape[0] == wide and args[7].shape[0] == wide
    fits = fits and hb % 64 == 0 and n // 2 == len(SUM_Y) and rows % hb == 0 and w % wide == 0
    return fused(n, *args) if fits else plain(*args)


def solution(mesh):
    in_specs = (
        P("replica", None, "model"),
        P("replica", "model", None),
        P("replica", None),
        P("replica", None),
        P("replica", "model"),
        P("model", "replica"),
        P("replica"),
        P("replica"),
        P("replica", "model"),
        P("model", "replica"),
        P("replica"),
        P("replica"),
    )
    out_specs = (
        P(None, "model"),
        P("model", None),
        P(),
        P(),
        P("replica", "model"),
        P("model", "replica"),
        P("replica"),
        P("replica"),
        P("replica", "model"),
        P("model", "replica"),
        P("replica"),
        P("replica"),
    )
    return jax.shard_map(
        on_device, mesh=mesh, in_specs=in_specs, out_specs=out_specs, check_vma=False
    )
```

```python
import functools
import math

import jax
import jax.numpy as jnp
from jax import lax
from jax.experimental import pallas as pl
from jax.experimental.pallas import tpu as pltpu
from jax.sharding import PartitionSpec as P

learn_rate = 0.05
hold_rate = 0.9


def plain(
    partial_up,
    partial_down,
    partial_norm,
    partial_bias,
    master_up,
    master_down,
    master_norm,
    master_bias,
    memory_up,
    memory_down,
    memory_norm,
    memory_bias,
):
    mean_up, mean_down = (
        lax.psum_scatter(partial_up[0], "replica", scatter_dimension=0, tiled=True),
        lax.psum_scatter(partial_down[0], "replica", scatter_dimension=1, tiled=True),
    )
    whole_norm, whole_bias = lax.psum((partial_norm[0], partial_bias[0]), "replica")
    place = lax.axis_index("replica")
    mean_norm = lax.dynamic_slice_in_dim(
        whole_norm, place * master_norm.shape[0], master_norm.shape[0]
    )
    mean_bias = lax.dynamic_slice_in_dim(
        whole_bias, place * master_bias.shape[0], master_bias.shape[0]
    )
    mean_rate = lax.axis_size("replica") ** (-0.5)
    mean_up = mean_up * mean_rate
    mean_down = mean_down * mean_rate
    mean_norm = mean_norm * mean_rate
    mean_bias = mean_bias * mean_rate
    state_new_up = hold_rate * memory_up + (1.0 - hold_rate) * mean_up * mean_up
    stepped_up = master_up - learn_rate * mean_up * lax.rsqrt(state_new_up + 1e-06)
    state_new_down = hold_rate * memory_down + (1.0 - hold_rate) * mean_down * mean_down
    stepped_down = master_down - learn_rate * mean_down * lax.rsqrt(state_new_down + 1e-06)
    state_new_norm = hold_rate * memory_norm + (1.0 - hold_rate) * mean_norm * mean_norm
    stepped_norm = master_norm - learn_rate * mean_norm * lax.rsqrt(state_new_norm + 1e-06)
    state_new_bias = hold_rate * memory_bias + (1.0 - hold_rate) * mean_bias * mean_bias
    stepped_bias = master_bias - learn_rate * mean_bias * lax.rsqrt(state_new_bias + 1e-06)
    compute_up, compute_down, compute_norm, compute_bias = (
        lax.all_gather(stepped_up.astype(jnp.bfloat16), "replica", axis=0, tiled=True),
        lax.all_gather(stepped_down.astype(jnp.bfloat16), "replica", axis=1, tiled=True),
        lax.all_gather(stepped_norm.astype(jnp.bfloat16), "replica", axis=0, tiled=True),
        lax.all_gather(stepped_bias.astype(jnp.bfloat16), "replica", axis=0, tiled=True),
    )
    return (
        compute_up,
        compute_down,
        compute_norm,
        compute_bias,
        stepped_up,
        stepped_down,
        stepped_norm,
        stepped_bias,
        state_new_up,
        state_new_down,
        state_new_norm,
        state_new_bias,
    )


SHARE = 3 / 4
SPAN = 124.0
POWER = 49
STEEP = 2.0 ** (2.0 * SPAN / POWER) - 1.0
LOW = 2.0 ** (-SPAN / POWER)
LAG_PAIR = 7
SUM_Y = (0, 4, 7, 10)
SUM_Z = (0, 4, 7, 11)
RELAY_Y = (0, 5, 8, 16)
RELAY_Z = (0, 21, 29, 48)
LAG_CLOSE = 4
LAG_SPREAD = 4
LAG_LAST = 2
LAG_VECTOR = 4
LAG_OWN = 4
LAG_NEAR = 9
HEAD_START = 2000
HOLD_Y = (1, 1, 0)
HOLD_Z = (14, 25, 0)
ORDER = ('rz', 'py', 'cy', 'a', 'cly', 'cz', 'spz', 'oz', 'clz', 'wy', 'oy', 'xz', 'f1', 'f', 'ry', 'ea')


def encode(x, reach):
    q = x * (LOW * STEEP / reach) + jnp.where(x < 0.0, -LOW, LOW)
    q2 = q * q
    q3 = q2 * q
    q6 = q3 * q3
    q12 = q6 * q6
    q24 = q12 * q12
    q48 = q24 * q24
    return (q48 * q).astype(jnp.bfloat16)


def decode(code, reach):
    y = code.astype(jnp.float32)
    grown = jnp.exp2(jnp.log(jnp.abs(y)) * (1.0 / (math.log(2.0) * POWER)))
    scale = reach / (LOW * STEEP)
    return (grown - LOW) * jnp.where(y < 0.0, -scale, scale)


def update(total, master, memory, rate):
    mean = total * rate
    state = hold_rate * memory + (1.0 - hold_rate) * mean * mean
    return master - learn_rate * mean * lax.rsqrt(state + 1e-06), state


def shares(hb):
    part_y = int(hb * SHARE) // 8 * 8
    cut_y, cut_z = -(-part_y // 32) * 16, (hb - part_y) // 32 * 16
    return (0, cut_y, part_y), (0, cut_z, hb - part_y)


def kernel(
    n,
    pu, pd, mu, md, su, sd, pn, pb, mn, mb, sn, sb,
    gy, gz, ou, od, qu, qd, cn, cb, step_s, state_s,
    xs, wu, wd, hu, hd,
    a_s, a_r, c_s0, c_s1, c_r0, c_r1, z_s0, z_s1, z_r0, z_r1, y_s, y_r,
    mine, theirs, packs, hold_s,
    sem_up, sem_down, sem_par, sem_vec,
    sa, ra, sc, rc, sz, rz, sy, ry, so, ro, st, rt, sf, rf, sg, rg, sp, rp, sq, rq, sv, rv, sw, rw,
):
    nz = n // 2
    tiles, _, hb, wide = xs.shape
    cuts_y, cuts_z = shares(hb)
    tiles_up = pu.shape[2] // wide
    me = lax.axis_index("replica")
    y = lax.rem(me, 2)
    row = lax.div(me, 2)
    other = me + 1 - 2 * y
    rate = n ** (-0.5)
    reach = n / 2.0
    c_s, c_r, z_s, z_r = (c_s0, c_s1), (c_r0, c_r1), (z_s0, z_s1), (z_r0, z_r1)

    def remote(src, dst, ss, rs, who):
        return pltpu.make_async_remote_copy(
            src_ref=src, dst_ref=dst, send_sem=ss, recv_sem=rs,
            device_id={"replica": who}, device_id_type=pl.DeviceIdType.MESH,
        )

    def load_up(k):
        lanes = pl.ds(pl.multiple_of(k * wide, wide), wide)
        return pltpu.make_async_copy(pu.at[:, :, lanes], xs.at[k], sem_up.at[k])

    def load_down(b):
        return pltpu.make_async_copy(
            pd.at[:, :, b * wide : (b + 1) * wide], xs.at[tiles_up:tiles, b], sem_down.at[b]
        )

    params = [
        pltpu.make_async_copy(a, b, sem_par.at[i])
        for i, (a, b) in enumerate(((mu, wu), (su, hu), (md, wd), (sd, hd)))
    ]
    vectors = [
        pltpu.make_async_copy(a, mine.at[at : at + a.shape[0], :], sem_vec.at[i])
        for i, (a, at) in enumerate(
            ((pn, 0), (pb, n), (mn, 2 * n), (mb, 2 * n + 1), (sn, 2 * n + 2), (sb, 2 * n + 3))
        )
    ]

    def rows_y(half):
        return slice(cuts_y[half], cuts_y[half + 1])

    def rows_z(half):
        return slice(cuts_z[half], cuts_z[half + 1])

    def rows_zx(half):
        return slice(cuts_y[2] + cuts_z[half], cuts_y[2] + cuts_z[half + 1])

    def encode_a(k, half):
        if half == 0:

            @pl.when(k < tiles_up)
            def _():
                load_up(k).wait()

            @pl.when(k == tiles_up)
            def _():
                for b in range(n):
                    load_down(b).wait()

        for t in range(nz):
            a_s[k, t, rows_y(half)] = encode(xs[k, 2 * t + 1 - y, rows_y(half), :], reach)

    load_up(0).start()
    barrier = pltpu.get_barrier_semaphore()
    pl.semaphore_signal(barrier, inc=1, device_id={"replica": other}, device_id_type=pl.DeviceIdType.MESH)

    @pl.when(row > 0)
    def _():
        pl.semaphore_signal(barrier, inc=1, device_id={"replica": me - 2}, device_id_type=pl.DeviceIdType.MESH)

    @pl.when(row < nz - 1)
    def _():
        pl.semaphore_signal(barrier, inc=1, device_id={"replica": me + 2}, device_id_type=pl.DeviceIdType.MESH)

    lax.fori_loop(1, tiles_up, lambda k, c: (load_up(k).start(), c)[1], 0)
    for p in params[:2]:
        p.start()
    mine[2 * n + 4 : 2 * n + 8, :] = jnp.zeros((4, wide), jnp.float32)
    for p in vectors:
        p.start()
    for b in range(n):
        load_down(b).start()
    for p in params[2:]:
        p.start()
    encode_a(jnp.int32(0), 0)

    def run(z):
        poses = (z, nz - 1 - z)
        far = max(poses)
        pl.semaphore_wait(barrier, 1 + (z > 0) + (z < nz - 1))
        pl.when(lax.rem(lax.axis_index("model"), 2) == 1)(lambda: pl.delay(HEAD_START))

        def beyond(d):
            return slice(z + 1, nz) if d == 0 else slice(0, z)

        def behind(d):
            return slice(0, z) if d == 0 else slice(z + 1, nz)

        def inward(d):
            return slice(z, nz) if d == 0 else slice(0, z + 1)

        def nextdev(d):
            return me + (2, -2)[d]

        def copy_a(k, half):
            r = rows_y(half)
            return remote(a_s.at[k, :, r], a_r.at[k, :, r], sa.at[0], ra.at[2 * k + half], other)

        def copy_c(k, half, d, sl):
            r = rows_y(half)
            return remote(c_s[d].at[k, sl, r], c_r[d].at[k, sl, r], sc.at[d], rc.at[d, 2 * k + half], nextdev(d))

        def copy_z(k, half, d, sl):
            r = rows_z(half)
            return remote(z_s[d].at[k, sl, :, r], z_r[d].at[k, sl, :, r], sz.at[d], rz.at[d, 2 * k + half], nextdev(d))

        def copy_y(k, half):
            r = rows_z(half)
            return remote(y_s.at[k, r], y_r.at[k, r], sy.at[0], ry.at[2 * k + half], other)

        def piece(ref, ss, rs, k, half, d):
            return remote(ref, ref, ss.at[d], rs.at[d, 2 * k + half], nextdev(d))

        def own_y(k, half, d, o):
            return piece(gy.at[k, o, y, rows_y(half)], so, ro, k, half, d)

        def rest_y(k, half, d, sl):
            return piece(gy.at[k, sl, y, rows_y(half)], st, rt, k, half, d)

        def fin_y(k, half, lo):
            ref = gy.at[k, lo : lo + 2, y, rows_y(half)]
            return remote(ref, ref, sf.at[0], rf.at[0], other)

        def side_z(k, half, who):
            ref = gz.at[k, z, who, rows_z(half)]
            return remote(ref, ref, sg.at[0], rg.at[2 * k + half], other)

        def own_z(k, half, d, o):
            return piece(gz.at[k, o, :, rows_z(half)], sp, rp, k, half, d)

        def rest_z(k, half, d, sl):
            return piece(gz.at[k, sl, :, rows_z(half)], sq, rq, k, half, d)

        def prior(d):
            return (z - 1, slice(0, z - 1)) if d == 0 else (z + 1, slice(z + 2, nz))

        def pair_y(k, half):
            r = rows_y(half)
            copy_a(k, half).wait_recv()
            for t in range(nz):
                at = (k, 2 * t + y, r)
                xs[at] = xs[at] + decode(a_r[k, t, r], reach)

        def chain_y(k, half, d):
            r = rows_y(half)
            pos = poses[d]
            if pos > 0:
                copy_c(k, half, d, inward(d)).wait_recv()
            for t in range(nz)[beyond(d)]:
                value = xs[k, 2 * t + y, r, :]
                if pos > 0:
                    value = value + decode(c_r[d][k, t, r], 2.0 * reach * pos)
                c_s[d][k, t, r] = encode(value, 2.0 * reach * (pos + 1))
            if pos < nz - 1:
                copy_c(k, half, d, beyond(d)).start()

        def finish(k, r, total, put, place):
            @pl.when(k < tiles_up)
            def _():
                spot = (r, pl.ds(pl.multiple_of(k * wide, wide), wide))
                stepped, state = update(total, wu[spot], hu[spot], rate)
                ou[spot] = stepped
                qu[spot] = state
                put[k, z, y, place] = stepped.astype(jnp.bfloat16)

            @pl.when(k >= tiles_up)
            def _():
                spot = pl.ds(pl.multiple_of((k - tiles_up) * hb + r.start, 8), r.stop - r.start)
                stepped, state = update(total, wd[spot, :], hd[spot, :], rate)
                od[spot, :] = stepped
                qd[spot, :] = state
                put[k, z, y, place] = stepped.astype(jnp.bfloat16)

        def close_y(k, half):
            r = rows_y(half)
            total = xs[k, me, r, :]
            for d in range(2):
                if poses[d] > 0:
                    total = total + decode(c_r[d][k, z, r], 2.0 * reach * poses[d])
            finish(k, r, total, gy, r)

        def send_y(k, half, d):
            own_y(k, half, d, z).start()

        def relay_y(k, half, d):
            pos = poses[d]
            sl = prior(d)[1]
            if pos > 1:
                rest_y(k, half, d, sl).wait_recv()
            if pos < nz - 1:
                rest_y(k, half, d, behind(d)).start()

        def heard_y(k, half, d):
            own_y(k, half, d, prior(d)[0]).wait_recv()

        def near_y(k, half):
            fin_y(k, half, z // 2 * 2).start()

        def last_y(k, half):
            for lo in range(0, nz, 2):
                if lo != z // 2 * 2:
                    fin_y(k, half, lo).start()

        def chain_z(k, half, d):
            r = rows_z(half)
            pos = poses[d]
            if pos > 0:
                copy_z(k, half, d, inward(d)).wait_recv()
            for t in range(nz)[beyond(d)]:
                for j in range(2):
                    value = xs[k, 2 * t + j, rows_zx(half), :]
                    if pos > 0:
                        value = value + decode(z_r[d][k, t, j, r], reach * pos)
                    z_s[d][k, t, j, r] = encode(value, reach * (pos + 1))
            if pos < nz - 1:
                copy_z(k, half, d, beyond(d)).start()

        def cross_z(k, half):
            r = rows_z(half)
            sums = []
            for who in (1 - y, y):
                total = xs[k, 2 * z + who, rows_zx(half), :]
                for d in range(2):
                    if poses[d] > 0:
                        total = total + decode(z_r[d][k, z, who, r], reach * poses[d])
                sums.append(total)
            y_s[k, r] = encode(sums[0], reach * nz)
            copy_y(k, half).start()
            xs[k, me, rows_zx(half), :] = sums[1]

        def close_z(k, half):
            r = rows_z(half)
            copy_y(k, half).wait_recv()
            total = xs[k, me, rows_zx(half), :] + decode(y_r[k, r], reach * nz)
            finish(k, rows_zx(half), total, gz, r)
            side_z(k, half, y).start()

        def spread_z(k, half):
            side_z(k, half, 1 - y).wait_recv()

        def send_z(k, half, d):
            own_z(k, half, d, z).start()

        def relay_z(k, half, d):
            pos = poses[d]
            o, sl = prior(d)
            own_z(k, half, d, o).wait_recv()
            if pos > 1:
                rest_z(k, half, d, sl).wait_recv()
            if pos < nz - 1:
                rest_z(k, half, d, behind(d)).start()

        def vec_send():
            for p in vectors:
                p.wait()
            remote(mine, theirs, sv.at[0], rv.at[0], other).start()

        def vec_pair():
            remote(mine, theirs, sv.at[0], rv.at[0], other).wait_recv()
            a, b = mine[...], theirs[...]
            packs[z, 0 : 2 * n, :] = a[0 : 2 * n, :] + b[0 : 2 * n, :]
            first = y == 0
            packs[z, 2 * n : 2 * n + 8, :] = jnp.concatenate(
                [
                    jnp.where(first, a[2 * n : 2 * n + 4, :], b[2 * n : 2 * n + 4, :]),
                    jnp.where(first, b[2 * n : 2 * n + 4, :], a[2 * n : 2 * n + 4, :]),
                ],
                axis=0,
            )

        def copy_v(d, sl):
            ref = packs.at[sl]
            return remote(ref, ref, sw.at[d], rw.at[d], nextdev(d))

        def through(d):
            return slice(0, z + 1) if d == 0 else slice(z, nz)

        def vec_chain(d):
            if poses[d] > 0:
                copy_v(d, behind(d)).wait_recv()
            if poses[d] < nz - 1:
                copy_v(d, through(d)).start()

        def vec_close():
            total = packs[0, 0 : 2 * n, :]
            for t in range(1, nz):
                total = total + packs[t, 0 : 2 * n, :]
            for t in range(nz):
                held = packs[t, 2 * n : 2 * n + 8, :]
                for j in range(2):
                    for i in range(4):
                        at = i * n + 2 * t + j
                        hold_s[at : at + 1, :] = held[4 * j + i : 4 * j + i + 1, :]
            stepped, state = update(total, hold_s[0 : 2 * n, :], hold_s[2 * n : 4 * n, :], rate)
            cn[...] = stepped[0:n].astype(jnp.bfloat16)
            cb[...] = stepped[n : 2 * n].astype(jnp.bfloat16)
            step_s[...] = stepped
            state_s[...] = state

        at_spread = LAG_PAIR + SUM_Y[nz - 1]
        at_close = LAG_PAIR + SUM_Y[far]
        side_sum = SUM_Z[far]
        side_close = side_sum + LAG_CLOSE
        side_open = side_close + LAG_SPREAD
        side_spread = SUM_Z[nz - 1] + LAG_CLOSE + LAG_SPREAD
        heard = {}
        for d in range(2):
            before = poses[d] - 1
            if before >= 0:
                heard[d] = LAG_PAIR + SUM_Y[max(before, nz - 1 - before)] + HOLD_Y[before] + LAG_OWN
        at_near = max(at_close, heard[1 - z % 2]) + LAG_NEAR
        tasks = {
            "wy": [(heard[d], functools.partial(heard_y, d=d)) for d in heard],
            "f1": [(at_near, near_y)],
            "a": [(0, lambda k, half: copy_a(k, half).start())],
            "ea": [(-1, encode_a)],
            "py": [(LAG_PAIR, pair_y)],
            "cy": [(LAG_PAIR + SUM_Y[poses[d]], functools.partial(chain_y, d=d)) for d in range(2)],
            "cly": [(at_close, close_y)],
            "oy": [(at_close + HOLD_Y[poses[d]], functools.partial(send_y, d=d)) for d in range(2) if poses[d] < nz - 1],
            "oz": [(side_open + HOLD_Z[poses[d]], functools.partial(send_z, d=d)) for d in range(2) if poses[d] < nz - 1],
            "ry": [(at_spread + RELAY_Y[poses[d]], functools.partial(relay_y, d=d)) for d in range(2) if poses[d] > 0],
            "f": [(at_spread + RELAY_Y[far] + LAG_LAST, last_y)],
            "cz": [(SUM_Z[poses[d]], functools.partial(chain_z, d=d)) for d in range(2)],
            "xz": [(side_sum, cross_z)],
            "clz": [(side_close, close_z)],
            "spz": [(side_open, spread_z)],
            "rz": [(side_spread + RELAY_Z[poses[d]], functools.partial(relay_z, d=d)) for d in range(2) if poses[d] > 0],
        }
        plan = [step for name in ORDER for step in tasks[name]]
        slots = 2 * tiles + max(lag for lag, _ in plan)
        vec_at = 2 + LAG_VECTOR
        extra = [(2, vec_send), (vec_at, vec_pair)]
        extra += [(vec_at + LAG_VECTOR * poses[d], functools.partial(vec_chain, d)) for d in range(2)]
        extra.append((vec_at + LAG_VECTOR * nz, vec_close))
        extra.append((min(at_close, side_close), lambda: [p.wait() for p in params] and None))

        def slot(v, carry):
            for i in range(2):
                for when, step in extra:
                    if when % 2 == i:
                        pl.when(v == when // 2)(step)

                for lag, task in plan:
                    half = (i - lag) % 2
                    k = v + (i - lag - half) // 2
                    pl.when(jnp.logical_and(k >= 0, k < tiles))(functools.partial(task, k, half))

            return carry

        lax.fori_loop(0, (slots + 1) // 2, slot, 0)

        remote(a_s, a_r, sa.at[0], ra.at[0], other).wait_send()
        for d in range(2):
            if poses[d] < nz - 1:
                remote(c_s[d].at[:, beyond(d)], c_r[d].at[:, beyond(d)], sc.at[d], rc.at[d, 0], other).wait_send()
                remote(z_s[d].at[:, beyond(d)], z_r[d].at[:, beyond(d)], sz.at[d], rz.at[d, 0], other).wait_send()
                ref = gy.at[:, z, y]
                remote(ref, ref, so.at[d], ro.at[d, 0], other).wait_send()
                ref = gz.at[:, z]
                remote(ref, ref, sp.at[d], rp.at[d, 0], other).wait_send()
                if poses[d] > 0:
                    ref = gy.at[:, behind(d), y]
                    remote(ref, ref, st.at[d], rt.at[d, 0], other).wait_send()
                    ref = gz.at[:, behind(d)]
                    remote(ref, ref, sq.at[d], rq.at[d, 0], other).wait_send()
                copy_v(d, through(d)).wait_send()
        remote(y_s, y_r, sy.at[0], ry.at[0], other).wait_send()
        ref = gz.at[:, z, y]
        remote(ref, ref, sg.at[0], rg.at[0], other).wait_send()
        remote(mine, theirs, sv.at[0], rv.at[0], other).wait_send()
        ref = gy.at[:, :, y]
        remote(ref, ref, sf.at[0], rf.at[0], other).wait_send()
        ref = gy.at[:, :, 1 - y]
        remote(ref, ref, sf.at[0], rf.at[0], other).wait_recv()

    for z in range(nz):
        pl.when(row == z)(functools.partial(run, z))


def leave(
    n, gy, gz, ou, od, qu, qd, cn, cb, step_s, state_s,
    cu, cd, tu, td, vu, vd, xcn, xcb, tn, tb, vn, vb, sem,
):
    me = lax.axis_index("replica")
    tiles, nz, _, part_y, wide = gy.shape
    tiles_up = cu.shape[3] // wide
    size = cu.shape[2]
    pairs = [(ou, tu), (od, td), (qu, vu), (qd, vd)]
    for ref, lo, hi in ((gy, 0, part_y), (gz, part_y, size)):
        for k in range(tiles_up):
            pairs.append((ref.at[k], cu.at[:, :, lo:hi, k * wide : (k + 1) * wide]))
        for b in range(n):
            pairs.append((ref.at[tiles_up:tiles, b // 2, b % 2], cd.at[:, lo:hi, b * wide : (b + 1) * wide]))
    pairs += [(cn, xcn), (cb, xcb)]
    pairs += [(step_s.at[pl.ds(me, 1), :], tn), (step_s.at[pl.ds(me + n, 1), :], tb)]
    pairs += [(state_s.at[pl.ds(me, 1), :], vn), (state_s.at[pl.ds(me + n, 1), :], vb)]
    copies = [pltpu.make_async_copy(a, b, sem.at[i]) for i, (a, b) in enumerate(pairs)]
    for c in copies:
        c.start()
    for c in copies:
        c.wait()


def fused(
    n, partial_up, partial_down, partial_norm, partial_bias, master_up, master_down,
    master_norm, master_bias, memory_up, memory_down, memory_norm, memory_bias,
):
    nz = n // 2
    hb, w = master_up.shape
    rows, wide = master_down.shape
    cuts_y, cuts_z = shares(hb)
    part_y, part_z = cuts_y[2], cuts_z[2]
    tiles_up, tiles_down = w // wide, rows // hb
    tiles = tiles_up + tiles_down
    units = tiles * 2
    f32, b16 = jnp.float32, jnp.bfloat16
    line = lambda a: a.reshape(1, -1)
    operands = (
        partial_up[0].reshape(n, hb, w), partial_down[0].reshape(tiles_down, hb, n * wide),
        master_up, master_down, memory_up, memory_down,
        partial_norm.reshape(n, -1), partial_bias.reshape(n, -1),
        line(master_norm), line(master_bias), line(memory_norm), line(memory_bias),
    )
    S = jax.ShapeDtypeStruct
    shapes = (
        S((nz, 2, hb, w), b16), S((tiles_down, hb, n * wide), b16),
        S((hb, w), f32), S((rows, wide), f32), S((hb, w), f32), S((rows, wide), f32),
        S((n, wide), b16), S((n, wide), b16),
        S((1, wide), f32), S((1, wide), f32), S((1, wide), f32), S((1, wide), f32),
    )
    hbm = pl.BlockSpec(memory_space=pltpu.HBM)
    vm = pl.BlockSpec(memory_space=pltpu.VMEM)
    D = pltpu.SemaphoreType.DMA
    V = pltpu.VMEM
    one, two, each, both = D((1,)), D((2,)), D((units,)), D((2, units))
    held = pl.pallas_call(
        functools.partial(kernel, n),
        out_shape=(
            S((tiles, nz, 2, part_y, wide), b16), S((tiles, nz, 2, part_z, wide), b16),
            S((hb, w), f32), S((rows, wide), f32), S((hb, w), f32), S((rows, wide), f32),
            S((n, wide), b16), S((n, wide), b16), S((2 * n, wide), f32), S((2 * n, wide), f32),
        ),
        in_specs=[hbm] * 12,
        out_specs=[vm] * 10,
        scratch_shapes=[
            V((tiles, n, hb, wide), f32),
            V((hb, w), f32), V((rows, wide), f32), V((hb, w), f32), V((rows, wide), f32),
            *[V((tiles, nz, part_y, wide), b16)] * 6,
            *[V((tiles, nz, 2, part_z, wide), b16)] * 4,
            *[V((tiles, part_z, wide), b16)] * 2,
            V((2 * n + 8, wide), f32), V((2 * n + 8, wide), f32), V((nz, 2 * n + 8, wide), f32), V((4 * n, wide), f32),
            D((tiles_up,)), D((n,)), D((4,)), D((6,)),
            one, each, two, both, two, both, one, each, two, both, two, both,
            one, one, one, each, two, both, two, both, one, one, two, two,
        ],
        compiler_params=pltpu.CompilerParams(
            collective_id=0, has_side_effects=True, vmem_limit_bytes=28 * 1024 * 1024
        ),
    )(*[pltpu.with_memory_space_constraint(a, pltpu.HBM) for a in operands])
    cu, cd, tu, td, vu, vd, cn, cb, tn, tb, vn, vb = pl.pallas_call(
        functools.partial(leave, n),
        out_shape=shapes,
        in_specs=[vm] * 10,
        out_specs=[hbm] * 12,
        scratch_shapes=[D((2 * (tiles_up + n) + 10,))],
        compiler_params=pltpu.CompilerParams(vmem_limit_bytes=4 * 1024 * 1024),
    )(*held)
    flat = lambda a: a.reshape(-1)
    return (
        cu.reshape(n * hb, w), cd.reshape(rows, n * wide), flat(cn), flat(cb),
        tu, td, flat(tn), flat(tb), vu, vd, flat(vn), flat(vb),
    )


def on_device(*args):
    n = lax.axis_size("replica")
    (hb, w), (rows, wide) = args[4].shape, args[5].shape
    fits = n % 8 == 0 and n < 16 and wide == 128 and args[6].shape[0] == wide and args[7].shape[0] == wide
    fits = fits and hb % 64 == 0 and n // 2 == len(SUM_Y) and rows % hb == 0 and w % wide == 0
    return fused(n, *args) if fits else plain(*args)


def solution(mesh):
    in_specs = (
        P("replica", None, "model"),
        P("replica", "model", None),
        P("replica", None),
        P("replica", None),
        P("replica", "model"),
        P("model", "replica"),
        P("replica"),
        P("replica"),
        P("replica", "model"),
        P("model", "replica"),
        P("replica"),
        P("replica"),
    )
    out_specs = (
        P(None, "model"),
        P("model", None),
        P(),
        P(),
        P("replica", "model"),
        P("model", "replica"),
        P("replica"),
        P("replica"),
        P("replica", "model"),
        P("model", "replica"),
        P("replica"),
        P("replica"),
    )
    return jax.shard_map(
        on_device, mesh=mesh, in_specs=in_specs, out_specs=out_specs, check_vma=False
    )
```
